32 devices in a mesh: col: 4 (over y, x), row: 8 (over z, core).
Axes of the slice: x: 2, y: 2, z: 4, core: 2. Of those that a mesh axis runs over, the one named last changes fastest.
Arguments:
- object_field: float32 [2, 4096, 2048], P(None, 'row', 'col'), may hold values from -20 to 20
- probe_field: float32 [2, 256, 256], replicated, may hold values from -4.2 to 4.2
- amplitudes: float32 [8, 4, 2, 256, 256], P('row', 'col'), may hold values from 0.25 to 2.5
- positions: int32 [8, 4, 2, 2], P('row', 'col'), may hold values from -128 to 384, as said below
- batch_order: int32 [8, 4, 2], P('row', 'col'), may hold values from 0 to 1, each once within a row
Outputs:
- object_out: float32 [2, 4096, 2048], P(None, 'row', 'col')
- probe_out: float32 [2, 256, 256], replicated
The draws below stay inside these ranges and needn't reach their ends.
Inputs may be any that keep to these rules, and one draw needn't show every extreme that they name: `positions`: in every tile some pattern's window reaches past its upper edge, some past its lower edge, some past its left edge and some past its right edge. `batch_order`: each tile's 2 entries name each of its patterns once.
All inputs are finite; a program needn't handle non-finite values.
Results may differ from the reference program's by a relative error of at most 0.0065.
Values sent between devices are 32-bit elements; how exact they have to be, the bound alone decides.
A program may use at most 128 MiB of HBM per device.

```python
import math
from functools import partial
import jax
import jax.numpy as jnp
from jax import lax

TILE = 512
W = 256
OV = 128
BS = 1
BATCHES = 2
EPOCHS = 1
PAT = 2
TROWS = 8
TCOLS = 4
NR = 4096
NC = 2048


def draw_object_field(key, part):
    noise_key, rough_key = jax.random.split(key, 2)
    row_frac = jnp.arange(NR, dtype=jnp.float32) / NR
    col_frac = jnp.arange(NC, dtype=jnp.float32) / NC
    trend = jnp.exp(0.5 * math.log(3.0) * (row_frac[:, None] + col_frac[None, :]))
    rough = jax.random.uniform(rough_key, (NR, NC), jnp.float32, 0.5, 1.5)
    base = jnp.clip(jax.random.normal(noise_key, (2, NR, NC), jnp.float32), -6.0, 6.0)
    return 0.7 * base * trend * rough


def draw_positions(key, part):
    depth_key, flip_key, free_key = jax.random.split(jax.random.fold_in(key, 7), 3)
    depth = jax.random.randint(depth_key, (TROWS, TCOLS, 2, PAT), 1, OV + 1, jnp.int32)
    flip = jax.random.randint(flip_key, (TROWS, TCOLS, 2, 1), 0, 2, jnp.int32)
    free = jax.random.randint(free_key, (TROWS, TCOLS, 2, PAT), 0 - OV, TILE - W + OV + 1, jnp.int32)
    index = jnp.arange(PAT, dtype=jnp.int32)[None, None, None, :]
    side = (index + flip) % 2
    edge = jnp.where(side == 0, 0 - depth, TILE - W + depth)
    return jnp.where(index < 2, edge, free).astype(jnp.int32)


def level_of(own_key, dims, shards, smallest, top_value):
    factor_of, own = 1.0, jax.random.fold_in(own_key, 6)
    for position, parts in shards:
        heights = jnp.exp(jax.random.uniform(jax.random.fold_in(own, position), (parts,), jnp.float32, smallest / len(shards), top_value / len(shards)))
        factor_of = factor_of * jnp.repeat(heights, dims[position] // parts).reshape([-1 if axis == position else 1 for axis in range(len(dims))])
    return factor_of


def gaussian(rng, extent, spread, reach, kind=jnp.bfloat16):
    entries = jax.random.normal(rng, extent, jnp.float32) * spread
    return jnp.minimum(jnp.maximum(entries, -reach), reach).astype(kind)


def setup_inputs(seed: int = 0) -> dict:
    streams_of = jax.random.split(jax.random.key(seed), 6)
    object_field = draw_object_field(jax.random.fold_in(streams_of[5], 71), 0)
    probe_field = gaussian(streams_of[1], (2, W, W), 0.7, 4.2, jnp.float32)
    amplitudes = jnp.clip(jnp.exp(math.log(2.5) - 2.3025851 * jax.random.uniform(streams_of[2], (TROWS, TCOLS, PAT, W, W), jnp.float32) ** level_of(streams_of[2], (TROWS, TCOLS, PAT, W, W), ((0, 8), (1, 4)), -0.2, 0.2)), 0.25, 2.5)
    positions = draw_positions(jax.random.fold_in(streams_of[5], 71), 0)
    batch_order = jax.vmap(lambda own: jax.random.permutation(own, PAT))(jax.random.split(streams_of[4], TROWS * TCOLS)).reshape((TROWS, TCOLS, PAT)).astype(jnp.int32)
    return dict(object_field=object_field, probe_field=probe_field, amplitudes=amplitudes, positions=positions, batch_order=batch_order)


ALPHA = 0.5
BETA = 4.0
FLOOR = 0.5
EPSILON = 1e-6


def to_tiles(field):
    return field.reshape(2, TROWS, TILE, TCOLS, TILE).transpose(0, 1, 3, 2, 4)


def from_tiles(tiled):
    return tiled.transpose(0, 1, 3, 2, 4).reshape(2, TROWS * TILE, TCOLS * TILE)


def extend(tiled):
    left_part = jnp.roll(tiled, 1, axis=2)[..., TILE - OV:]
    right_part = jnp.roll(tiled, -1, axis=2)[..., :OV]
    widened = jnp.concatenate([left_part, tiled, right_part], axis=-1)
    upper_part = jnp.roll(widened, 1, axis=1)[..., TILE - OV:, :]
    lower_part = jnp.roll(widened, -1, axis=1)[..., :OV, :]
    return jnp.concatenate([upper_part, widened, lower_part], axis=-2)


def fold_columns(grads):
    own_rows = grads[..., OV:OV + TILE]
    own_rows = own_rows.at[..., :OV].add(jnp.roll(grads[..., OV + TILE:], 1, axis=2))
    own_rows = own_rows.at[..., TILE - OV:].add(jnp.roll(grads[..., :OV], -1, axis=2))
    return own_rows


def tile_gradient(probe_now, batch_index, inputs):
    extended, tile_pos, tile_order, tile_amps = inputs
    picked = tile_order[batch_index * BS:(batch_index + 1) * BS]
    row_pos = tile_pos[0][picked] + OV
    col_pos = tile_pos[1][picked] + OV
    amp_rows = tile_amps[picked]
    zero = jnp.zeros((), jnp.int32)
    windows = jnp.stack([lax.dynamic_slice(extended, (zero, row_pos[member], col_pos[member]), (2, W, W)) for member in range(BS)], axis=1)
    win_re = windows[0]
    win_im = windows[1]
    probe_re = probe_now[0]
    probe_im = probe_now[1]
    wave = lax.complex(probe_re * win_re - probe_im * win_im, probe_re * win_im + probe_im * win_re)
    far_field = jnp.fft.fft2(wave, norm="ortho")
    modulus = jnp.abs(far_field)
    resid = far_field - (amp_rows / jnp.maximum(modulus, FLOOR)) * far_field
    back = jnp.fft.ifft2(resid, norm="ortho")
    back_re = jnp.real(back)
    back_im = jnp.imag(back)
    object_terms = jnp.stack([probe_re * back_re + probe_im * back_im, probe_re * back_im - probe_im * back_re])
    probe_terms = jnp.stack([jnp.sum(win_re * back_re + win_im * back_im, axis=0), jnp.sum(win_re * back_im - win_im * back_re, axis=0)])
    gradient = jnp.zeros_like(extended)
    for member in range(BS):
        start = (zero, row_pos[member], col_pos[member])
        current = lax.dynamic_slice(gradient, start, (2, W, W))
        gradient = lax.dynamic_update_slice(gradient, current + object_terms[:, member], start)
    return gradient, probe_terms


def reference(object_field, probe_field, amplitudes, positions, batch_order):
    span_ext = TILE + 2 * OV
    field_now = to_tiles(object_field)
    probe_now = probe_field
    flat_pos = positions.reshape(TROWS * TCOLS, 2, PAT)
    flat_order = batch_order.reshape(TROWS * TCOLS, PAT)
    flat_amps = amplitudes.reshape(TROWS * TCOLS, PAT, W, W)
    for epoch_index in range(EPOCHS):
        power_total = jnp.sum(field_now * field_now)
        step_object = ALPHA / (jnp.mean(probe_now[0] * probe_now[0] + probe_now[1] * probe_now[1]) + EPSILON)
        deferred = jnp.zeros_like(field_now)
        probe_sum = jnp.zeros_like(probe_now)
        for batch_index in range(BATCHES):
            extended = extend(field_now).transpose(1, 2, 0, 3, 4).reshape(TROWS * TCOLS, 2, span_ext, span_ext)
            grads, probe_terms = lax.map(partial(tile_gradient, probe_now, batch_index), (extended, flat_pos, flat_order, flat_amps))
            grads = grads.reshape(TROWS, TCOLS, 2, span_ext, span_ext).transpose(2, 0, 1, 3, 4)
            probe_sum = probe_sum + jnp.sum(probe_terms, axis=0)
            immediate = fold_columns(grads[..., OV:OV + TILE, :])
            upper_band = fold_columns(grads[..., :OV, :])
            lower_band = fold_columns(grads[..., OV + TILE:, :])
            deferred = deferred.at[..., TILE - OV:, :].add(jnp.roll(upper_band, -1, axis=1))
            deferred = deferred.at[..., :OV, :].add(jnp.roll(lower_band, 1, axis=1))
            field_now = field_now - step_object * immediate
        field_now = field_now - step_object * deferred
        cell_count = NR * NC
        mean_power = power_total / cell_count + EPSILON
        step_probe = BETA * W * W / (cell_count * mean_power)
        probe_now = probe_now - step_probe * probe_sum
    return from_tiles(field_now), probe_now
```

```python
import functools
import math

import jax
import jax.numpy as jnp
import numpy as np
from jax import lax
from jax.experimental import pallas as pl
from jax.experimental.pallas import tpu as pltpu
from jax.sharding import PartitionSpec as P

OV = 128

ALPHA = 0.5
BETA = 4.0
FLOOR = 0.5
EPSILON = 1e-06

UP, DOWN, LEFT, RIGHT = 0, 1, 2, 3
CHUNKS = 4


def dft_tables(size_w):
    counter = np.arange(size_w)
    angles = 2.0 * math.pi / size_w * (counter[:, None] * counter[None, :] % size_w)
    both = np.concatenate([np.cos(angles), np.sin(angles)], axis=1) / math.sqrt(size_w)
    both = both.astype(np.float32)
    head = both.astype(jnp.bfloat16)
    rest = (both - head.astype(np.float32)).astype(jnp.bfloat16)
    return head, rest


def halves(value):
    head = value.astype(jnp.bfloat16)
    rest = (value - head.astype(jnp.float32)).astype(jnp.bfloat16)
    return head, rest


def dot(left, right):
    return jnp.dot(left, right, preferred_element_type=jnp.float32)


def left_apply(tab_head, tab_rest, re_part, im_part, sign):
    size = re_part.shape[0]
    head, rest = halves(jnp.concatenate([re_part, im_part], axis=1))
    out = dot(tab_head, head) + dot(tab_head, rest) + dot(tab_rest, head)
    cos_re, cos_im = out[:size, :size], out[:size, size:]
    sin_re, sin_im = out[size:, :size], out[size:, size:]
    return cos_re + sign * sin_im, cos_im - sign * sin_re


def right_apply(re_part, im_part, tab_head, tab_rest, sign):
    size = re_part.shape[0]
    head, rest = halves(jnp.concatenate([re_part, im_part], axis=0))
    out = dot(head, tab_head) + dot(rest, tab_head) + dot(head, tab_rest)
    re_cos, re_sin = out[:size, :size], out[:size, size:]
    im_cos, im_sin = out[size:, :size], out[size:, size:]
    return re_cos + sign * im_sin, im_cos - sign * re_sin


def pick(flag, first, second):
    return jnp.where(flag == 1, first, second)


def keep(flag, value):
    return jnp.where(flag == 1, value, 0.0)


def across(*parts):
    return jnp.concatenate(parts, axis=1)


def stacked(*parts):
    return jnp.concatenate(parts, axis=0)


class Spot:
    def __init__(self, row, col, tile):
        half = tile // 2
        inside = lambda place: jnp.where(
            place < 0, jnp.maximum(place, -OV), jnp.clip(place, half, half + OV)
        )
        row, col = inside(row), inside(col)
        self.row, self.col = row, col
        self.up = jnp.where(row < 0, 1, 0)
        self.left = jnp.where(col < 0, 1, 0)
        self.row_on = jnp.where(row < 0, row + OV, row - half)
        self.col_on = jnp.where(col < 0, col + OV, col - half)


def choose(flag, first, second, tile):
    return Spot(
        jnp.where(flag == 1, first.row, second.row),
        jnp.where(flag == 1, first.col, second.col),
        tile,
    )


def same(first, second):
    return 1 - (first - second) * (first - second)


def kernel(
    rows, cols, pos, order, obj, probe_in, amps_in, lh_in, lr_in, rh_in, rr_in,
    out, probe_out,
    own, rim, mid, probe, amps, lh, lr, rh, rr, info, infos, hs, hr, vbuf, placed,
    bs, br, bnd_s, bnd_r, dreg, cs, cr, mid_s, mid_r, rim_s, rim_r,
    psum, acc, rx0, rx1, red, rx2, res, pw, pw0, pwa, pw1, pw2,
    local_sems, send_sems, recv_sems,
):
    tile = own.shape[2]
    blocks = tile // OV
    size_w = probe.shape[-1]
    half = tile // 2
    span = half + OV
    row, col = lax.axis_index("row"), lax.axis_index("col")
    core, par = row % 2, col % 2
    at = lambda r, c: {"row": r, "col": c}
    above, below = at((row + rows - 1) % rows, col), at((row + 1) % rows, col)
    west, east = at(row, (col + cols - 1) % cols), at(row, (col + 1) % cols)
    partner = at(row, col + 1 - 2 * par)
    onward = at(row, (col + 2 - 4 * par + cols) % cols)
    sibling = at(row + 1 - 2 * core, col)
    used = [0, 0]

    def fetch(source, target):
        copy = pltpu.make_async_copy(source, target, local_sems.at[used[0]])
        used[0] += 1
        copy.start()
        return copy

    def send(source, target, device):
        copy = pltpu.make_async_remote_copy(
            src_ref=source,
            dst_ref=target,
            send_sem=send_sems.at[used[1]],
            recv_sem=recv_sems.at[used[1]],
            device_id=device,
            device_id_type=pl.DeviceIdType.MESH,
        )
        used[1] += 1
        copy.start()
        sent.append(copy)
        return copy

    sent = []
    lanes = [pl.ds(block * OV, OV) for block in range(blocks)]
    own_in = [fetch(obj.at[:, :, lanes[block]], own.at[:, block]) for block in range(blocks)]
    rim_in = [
        fetch(obj.at[:, :, lanes[block]], rim.at[side, :, pl.ds(OV, tile), :])
        for side, block in ((0, 0), (1, blocks - 1))
    ]
    tall_in = [
        fetch(obj.at[:, :, lanes[block]], mid.at[block - 1, :, pl.ds(OV, tile), :])
        for block in range(1, blocks - 1)
    ]
    rest_in = [
        fetch(source, target)
        for source, target in (
            (probe_in, probe), (lh_in, lh), (lr_in, lr), (rh_in, rh), (rr_in, rr), (amps_in, amps),
        )
    ]

    mine = []
    for batch in range(2):
        which = order[batch]
        info[2 * batch] = pos[0, which]
        info[2 * batch + 1] = pos[1, which]
        mine.append(Spot(pos[0, which], pos[1, which], tile))

    barrier = pltpu.get_barrier_semaphore()
    peers = [above, below]
    peers += [at(row, (col + d) % cols) for d in range(1, cols)]
    peers += [at((row + 2 * d) % rows, col) for d in range(1, rows // 2)]
    for peer in peers:
        pl.semaphore_signal(barrier, inc=1, device_id=peer, device_id_type=pl.DeviceIdType.MESH)
    pl.semaphore_wait(barrier, len(peers))

    info_in = {}
    for peer, slot in ((west, RIGHT), (east, LEFT), (above, DOWN), (below, UP)):
        info_in[slot] = send(info, infos.at[slot], peer)
    side_block = (0, blocks - 1)
    edge_in, mid_in = [], []

    def send_past(block, tall):
        return [
            send(obj.at[:, pl.ds(0, OV), lanes[block]], tall.at[:, pl.ds(OV + tile, OV), :], above),
            send(obj.at[:, pl.ds(tile - OV, OV), lanes[block]], tall.at[:, pl.ds(0, OV), :], below),
        ]

    for side in range(2):
        edge_in += send_past(side_block[side], rim.at[side])
    for block in range(1, blocks - 1):
        mid_in += send_past(block, mid.at[block - 1])

    for copy in own_in:
        copy.wait()
    for index in range(4):
        for block in range(span // OV):
            gap = jnp.zeros((OV, OV), jnp.float32)
            placed[index, block, pl.ds(0, OV), :] = gap
            placed[index, block, pl.ds(OV + size_w, OV), :] = gap

    near = {}

    def spots(slot):
        info_in[slot].wait_recv()
        near[slot] = [Spot(infos[slot, 2 * b], infos[slot, 2 * b + 1], tile) for b in range(2)]

    spots(LEFT)
    spots(RIGHT)
    west_first = 1 - near[LEFT][0].left
    east_first = near[RIGHT][0].left
    west_spot = choose(west_first, near[LEFT][0], near[LEFT][1], tile)
    east_spot = choose(east_first, near[RIGHT][0], near[RIGHT][1], tile)
    wanted = (west_spot, east_spot)

    halo_in = {}
    for side in range(2):
        spot = wanted[side]
        start = jnp.where(spot.up == 1, spot.row + OV, spot.row)
        for part in range(2):
            hs[side, 0, part] = own[part, side_block[side], pl.ds(start, OV), :]
        halo_in[1 - side, 0] = send(
            hs.at[side, 0], hr.at[1 - side, 0], (west, east)[side]
        )

    squares = jnp.zeros((8, OV), jnp.float32)
    for part in range(2):
        for block in range(blocks):
            value = own[part, block]
            squares = squares + jnp.sum((value * value).reshape(tile // 8, 8, OV), axis=0)
    pw[...] = squares

    for copy in edge_in:
        copy.wait_recv()
    for copy in rim_in:
        copy.wait()
    for side in range(2):
        spot = wanted[side]
        start = jnp.where(spot.up == 1, spot.row + OV, spot.row + 2 * OV)
        for part in range(2):
            hs[side, 1, part] = rim[side, part, pl.ds(start, OV), :]
        halo_in[1 - side, 1] = send(
            hs.at[side, 1], hr.at[1 - side, 1], (west, east)[side]
        )

    for copy in mid_in:
        copy.wait_recv()
    for copy in tall_in:
        copy.wait()
    for copy in rest_in:
        copy.wait()
    spots(UP)
    spots(DOWN)
    power_probe = jnp.sum(
        probe[0] * probe[0] + probe[1] * probe[1], axis=(0, 1), keepdims=True
    )
    step_object = ALPHA / (power_probe / float(size_w * size_w) + EPSILON)

    def cut(value, spot):
        back = jnp.where(spot.col_on == 0, 0, span - spot.col_on)
        return pltpu.roll(value, back, 1)[:, :size_w]

    for copy in halo_in.values():
        copy.wait_recv()
    for batch in range(2):
        spot = mine[batch]
        for part in range(2):
            first = pick(spot.left, hr[0, 0, part], hr[1, 0, part])
            second = pick(spot.left, hr[0, 1, part], hr[1, 1, part])
            strip = pick(spot.up, stacked(second, first), stacked(first, second))
            window = pl.ds(spot.row + OV, size_w)
            tall = [rim[0, part, window, :]]
            tall += [mid[block - 1, part, window, :] for block in range(1, blocks - 1)]
            tall.append(rim[1, part, window, :])
            near_half = half // OV
            body = pick(spot.left, across(*tall[:near_half]), across(*tall[near_half:]))
            region = pick(spot.left, across(strip, body), across(body, strip))
            vbuf[2 * batch + part] = cut(region, spot)

    def transform(batch):
        spot = mine[batch]
        win_re, win_im = vbuf[2 * batch], vbuf[2 * batch + 1]
        probe_re, probe_im = probe[0], probe[1]
        exit_re = probe_re * win_re - probe_im * win_im
        exit_im = probe_re * win_im + probe_im * win_re
        half_re, half_im = left_apply(lh[...], lr[...], exit_re, exit_im, 1.0)
        far_re, far_im = right_apply(half_re, half_im, rh[...], rr[...], 1.0)
        modulus = jnp.sqrt(far_re * far_re + far_im * far_im)
        scaled = amps[order[batch]] / jnp.maximum(modulus, FLOOR)
        half_re, half_im = left_apply(
            lh[...], lr[...], far_re - scaled * far_re, far_im - scaled * far_im, -1.0
        )
        back_re, back_im = right_apply(half_re, half_im, rh[...], rr[...], -1.0)
        terms = (
            win_re * back_re + win_im * back_im,
            win_re * back_im - win_im * back_re,
        )
        for part in range(2):
            psum[part] = terms[part] if batch == 0 else psum[part] + terms[part]
        moves = (
            probe_re * back_re + probe_im * back_im,
            probe_re * back_im - probe_im * back_re,
        )
        beside = jnp.zeros((size_w, span - size_w), jnp.float32)
        for part in range(2):
            wide = across(step_object * moves[part], beside)
            wide = pltpu.roll(wide, spot.col_on, 1)
            for block in range(span // OV):
                placed[2 * batch + part, block, pl.ds(OV, size_w), :] = wide[:, block * OV : (block + 1) * OV]

    def load_placed(index, start, count):
        rows_of = pl.ds(start, count)
        return across(*[placed[index, block, rows_of, :] for block in range(span // OV)])

    def frame(batch, part, kind):
        spot = mine[batch]
        upper, lower = {"past": (-OV, tile), "edge": (0, tile - OV), "deep": (OV, half)}[kind]
        start = OV - spot.row + jnp.where(spot.up == 1, upper, lower)
        return load_placed(2 * batch + part, start, OV)

    transform(0)

    split = 2 * OV // CHUNKS
    per = OV // split
    block_in, block_on = [], []
    spot = mine[0]
    for chunk in range(CHUNKS):
        kind = ("edge", "deep")[chunk // per]
        low = (chunk % per) * split
        for part in range(2):
            value = frame(0, part, kind)[low : low + split]
            bs[chunk, part] = pick(spot.left, value[:, : 2 * OV], value[:, span - 2 * OV :])
        block_in.append(send(bs.at[chunk], br.at[par, chunk], partner))

    def hand_on(copy, buffer, index):
        copy.wait_recv()
        return send(buffer.at[1 - par, index], buffer.at[par, index], onward)

    for part in range(2):
        value = frame(0, part, "past")
        cs[0, part] = pick(spot.left, value[:, :OV], value[:, span - OV :])
    for chunk in range(per):
        block_on.append(hand_on(block_in[chunk], br, chunk))
    corner_in = [send(cs.at[0], cr.at[par, 0], partner)]
    for copy in block_on:
        copy.wait_recv()

    def near_block(side, part, kind):
        base = 0 if kind == "edge" else per
        return stacked(*[br[side, base + k, part] for k in range(per)])

    toward = (1 - near[LEFT][0].left, near[RIGHT][0].left)
    blank = jnp.zeros((OV, span - 2 * OV), jnp.float32)
    band_in = []
    for way, slot in ((0, UP), (1, DOWN)):
        goal = near[slot][1]
        match = spot.up if way == 0 else 1 - spot.up
        use_own = match * same(spot.left, goal.left)
        ups = [near[LEFT][0].up, near[RIGHT][0].up]
        if way == 1:
            ups = [1 - flag for flag in ups]
        use = jnp.where(goal.left == 1, ups[0] * toward[0], ups[1] * toward[1])
        for part in range(2):
            block = pick(goal.left, near_block(0, part, "edge"), near_block(1, part, "edge"))
            block = keep(use, block)
            whole = keep(use_own, frame(0, part, "edge"))
            whole = whole + pick(goal.left, across(block, blank), across(blank, block))
            bnd_s[way, part] = cut(whole, goal)
        band_in.append(
            send(bnd_s.at[way], bnd_r.at[1 - way], (above, below)[way])
        )
    for chunk in range(per, CHUNKS):
        block_on.append(hand_on(block_in[chunk], br, chunk))
    corner_on = [hand_on(corner_in[0], cr, 0)]
    for copy in block_on[per:]:
        copy.wait_recv()

    spot = mine[1]
    use = jnp.where(
        spot.left == 1,
        toward[0] * same(near[LEFT][0].up, spot.up),
        toward[1] * same(near[RIGHT][0].up, spot.up),
    )
    wide_blank = jnp.zeros((half, span - 2 * OV), jnp.float32)
    inside = []
    for part in range(2):
        at_edge = pick(spot.left, near_block(0, part, "edge"), near_block(1, part, "edge"))
        deep = pick(spot.left, near_block(0, part, "deep"), near_block(1, part, "deep"))
        block = keep(use, pick(spot.up, stacked(at_edge, deep), stacked(deep, at_edge)))
        inside.append(cut(pick(spot.left, across(block, wide_blank), across(wide_blank, block)), spot))
    for copy in band_in:
        copy.wait_recv()
    for part in range(2):
        band = pick(spot.up, bnd_r[0, part], bnd_r[1, part])
        region = pick(spot.up, stacked(band, inside[part]), stacked(inside[part], band))
        for block in range(size_w // OV):
            dreg[part, block] = region[:, block * OV : (block + 1) * OV]
    for part in range(2):
        change = [dreg[part, b, pl.ds(spot.row_on, size_w), :] for b in range(size_w // OV)]
        vbuf[2 + part] = vbuf[2 + part] - across(*change)

    transform(1)

    pair_in = send(psum.at[1 - core], rx0, sibling)
    power_in = [send(pw, pw0, sibling)]

    for index, kind in ((1, "past"), (2, "edge"), (3, "deep")):
        for part in range(2):
            value = frame(1, part, kind)
            cs[index, part] = pick(spot.left, value[:, :OV], value[:, span - OV :])
    pair_in.wait_recv()
    acc[...] = psum[core] + rx0[...]
    power_in[0].wait_recv()
    pwa[...] = pw[...] + pw0[...]
    piece = size_w // cols
    part_in = []
    for step in range(1, cols):
        other = (col + step) % cols
        part_in.append(
            send(acc.at[pl.ds(other * piece, piece)], rx1.at[step - 1], at(row, other))
        )
        power_in.append(send(pwa, pw1.at[col], at(row, other)))
    for index in range(1, 4):
        corner_in.append(send(cs.at[index], cr.at[par, index], partner))

    first_up = mine[0].up
    out_spots = (
        choose(first_up, mine[0], mine[1], tile),
        choose(first_up, mine[1], mine[0], tile),
    )
    out_batch = (1 - first_up, first_up)
    up_start = jnp.maximum(OV - out_spots[0].row, OV)

    def wide_own(way, part, start, count):
        value = load_placed(2 * out_batch[way] + part, start, count)
        left = out_spots[way].left
        body = pick(left, value[:, OV:], value[:, :half])
        gap = jnp.zeros((count, half), jnp.float32)
        return pick(left, across(body, gap), across(gap, body))

    past_in = []
    for way in range(2):
        start = up_start - OV if way == 0 else OV + tile - out_spots[1].row
        for part in range(2):
            value = wide_own(way, part, start, OV)
            mid_s[way, part] = value[:, OV : tile - OV]
            rim_s[way, 0, part] = value[:, :OV]
            rim_s[way, 1, part] = value[:, tile - OV :]

    mine_piece = acc[pl.ds(pl.multiple_of(col * piece, piece), piece), :]
    for copy in part_in:
        copy.wait_recv()
    for step in range(cols - 1):
        mine_piece = mine_piece + rx1[step]
    red[...] = mine_piece
    for copy in power_in[1:]:
        copy.wait_recv()
    pw1[col] = pwa[...]
    total = pw1[0]
    for place in range(1, cols):
        total = total + pw1[place]
    pw2[rows // 2] = total
    plane = row // 2
    plane_in = []
    for step in range(1, rows // 2):
        goal = at((row + 2 * step) % rows, col)
        plane_in.append(send(red, rx2.at[plane], goal))
        plane_in.append(send(pw2.at[rows // 2], pw2.at[plane], goal))
    for way in range(2):
        past_in.append(send(mid_s.at[way], mid_r.at[1 - way], (above, below)[way]))

    corner_on.append(hand_on(corner_in[1], cr, 1))
    corner_on.append(hand_on(corner_in[2], cr, 2))
    corner_on.append(hand_on(corner_in[3], cr, 3))

    for copy in plane_in:
        copy.wait_recv()
    rx2[plane] = red[...]
    pw2[plane] = total
    whole, total = rx2[0], pw2[0]
    for place in range(1, rows // 2):
        whole = whole + rx2[place]
        total = total + pw2[place]
    here = pl.ds(pl.multiple_of(col * piece, piece), piece)
    res[core, here, :] = whole
    gather_in = []
    for step in range(1, cols):
        other = at(row, (col + step) % cols)
        gather_in.append(send(res.at[core, here], res.at[core, here], other))

    corner_on[0].wait_recv()
    corner_on[1].wait_recv()
    for way in range(2):
        for side in range(2):
            theirs = wanted[side]
            first = (west_first, east_first)[side]
            match = theirs.up if way == 0 else 1 - theirs.up
            for part in range(2):
                corner = pick(first, cr[side, 0, part], cr[side, 1, part])
                rim_s[way, side, part] = rim_s[way, side, part] + keep(match, corner)
    for way in range(2):
        past_in.append(send(rim_s.at[way], rim_r.at[1 - way], (above, below)[way]))

    for copy in gather_in:
        copy.wait_recv()
    last_in = send(res.at[core], res.at[core], sibling)

    corner_on[2].wait_recv()
    corner_on[3].wait_recv()
    for copy in past_in:
        copy.wait_recv()
    gap = jnp.zeros((half, tile - 2 * OV), jnp.float32)
    for part in range(2):
        outer = []
        for side in range(2):
            first = (west_first, east_first)[side]
            part_of = slice(OV, 2 * OV) if side == 0 else slice(0, OV)
            at_edge = pick(first, near_block(side, part, "edge")[:, part_of], cr[side, 2, part])
            deep = pick(first, near_block(side, part, "deep")[:, part_of], cr[side, 3, part])
            up = wanted[side].up
            outer.append((up, at_edge, deep))
        for way in range(2):
            start = up_start if way == 0 else OV + half - out_spots[1].row
            value = wide_own(way, part, start, half)
            strips = []
            for up, at_edge, deep in outer:
                flag = up if way == 0 else 1 - up
                strips.append(
                    keep(flag, stacked(at_edge, deep) if way == 0 else stacked(deep, at_edge))
                )
            value = value + across(strips[0], gap, strips[1])
            late = across(rim_r[way, 0, part], mid_r[way, part], rim_r[way, 1, part])
            rest = jnp.zeros((half - OV, tile), jnp.float32)
            value = value + (stacked(late, rest) if way == 0 else stacked(rest, late))
            band = pl.ds(way * half, half)
            old = across(*[own[part, block, band, :] for block in range(blocks)])
            out[part, band, :] = old - value

    last_in.wait_recv()
    cell_count = float(tile * tile * rows * cols)
    mean_power = jnp.sum(total, axis=(0, 1), keepdims=True) / cell_count + EPSILON
    step_probe = BETA * size_w * size_w / (cell_count * mean_power)
    for part in range(2):
        probe_out[part] = probe[part] - step_probe * res[part]
    for copy in sent:
        copy.wait_send()


def local(mesh_shape, object_field, probe_field, amplitudes, positions, batch_order):
    rows, cols = mesh_shape["row"], mesh_shape["col"]
    size_w = probe_field.shape[-1]
    tile = object_field.shape[1]
    half = tile // 2
    span = half + OV
    head, rest = dft_tables(size_w)
    f32 = lambda *shape: pltpu.VMEM(shape, jnp.float32)
    b16 = lambda *shape: pltpu.VMEM(shape, jnp.bfloat16)
    piece = size_w // cols
    split = 2 * OV // CHUNKS
    scratch = dict(
        own=f32(2, tile // OV, tile, OV),
        rim=f32(2, 2, tile + 2 * OV, OV),
        mid=f32(tile // OV - 2, 2, tile + 2 * OV, OV),
        probe=f32(2, size_w, size_w),
        amps=f32(2, size_w, size_w),
        lh=b16(2 * size_w, size_w),
        lr=b16(2 * size_w, size_w),
        rh=b16(size_w, 2 * size_w),
        rr=b16(size_w, 2 * size_w),
        info=pltpu.SMEM((4,), jnp.int32),
        infos=pltpu.SMEM((4, 4), jnp.int32),
        hs=f32(2, 2, 2, OV, OV),
        hr=f32(2, 2, 2, OV, OV),
        vbuf=f32(4, size_w, size_w),
        placed=f32(4, span // OV, size_w + 2 * OV, OV),
        bs=f32(CHUNKS, 2, split, 2 * OV),
        br=f32(2, CHUNKS, 2, split, 2 * OV),
        bnd_s=f32(2, 2, OV, size_w),
        bnd_r=f32(2, 2, OV, size_w),
        dreg=f32(2, size_w // OV, span, OV),
        cs=f32(4, 2, OV, OV),
        cr=f32(2, 4, 2, OV, OV),
        mid_s=f32(2, 2, OV, tile - 2 * OV),
        mid_r=f32(2, 2, OV, tile - 2 * OV),
        rim_s=f32(2, 2, 2, OV, OV),
        rim_r=f32(2, 2, 2, OV, OV),
        psum=f32(2, size_w, size_w),
        acc=f32(size_w, size_w),
        rx0=f32(size_w, size_w),
        rx1=f32(cols - 1, piece, size_w),
        red=f32(piece, size_w),
        rx2=f32(rows // 2, piece, size_w),
        res=f32(2, size_w, size_w),
        pw=f32(8, 128),
        pw0=f32(8, 128),
        pwa=f32(8, 128),
        pw1=f32(cols, 8, 128),
        pw2=f32(rows // 2 + 1, 8, 128),
    )
    sends = 96 + 4 * cols + 2 * rows
    hbm = pl.BlockSpec(memory_space=pl.ANY)
    vmem = pl.BlockSpec(memory_space=pltpu.VMEM)
    smem = pl.BlockSpec(memory_space=pltpu.SMEM)
    dma = pltpu.SemaphoreType.DMA
    return pl.pallas_call(
        functools.partial(kernel, rows, cols),
        out_shape=(
            jax.ShapeDtypeStruct(object_field.shape, jnp.float32),
            jax.ShapeDtypeStruct(probe_field.shape, jnp.float32),
        ),
        in_specs=[smem, smem] + [hbm] * 7,
        out_specs=(vmem, vmem),
        scratch_shapes=list(scratch.values()) + [dma((32,)), dma((sends,)), dma((sends,))],
        compiler_params=pltpu.CompilerParams(
            collective_id=0, has_side_effects=True, vmem_limit_bytes=56 * 1024 * 1024
        ),
    )(
        positions[0, 0],
        batch_order[0, 0],
        object_field,
        probe_field,
        amplitudes[0, 0],
        jnp.asarray(np.concatenate(np.split(head, 2, axis=1), axis=0)),
        jnp.asarray(np.concatenate(np.split(rest, 2, axis=1), axis=0)),
        jnp.asarray(head),
        jnp.asarray(rest),
    )


def solution(mesh):
    return jax.shard_map(
        functools.partial(local, dict(mesh.shape)),
        mesh=mesh,
        in_specs=(
            P(None, "row", "col"),
            P(),
            P("row", "col", None, None, None),
            P("row", "col", None, None),
            P("row", "col", None),
        ),
        out_specs=(P(None, "row", "col"), P()),
        check_vma=False,
    )
```

```python
import functools
import math

import jax
import jax.numpy as jnp
import numpy as np
from jax import lax
from jax.experimental import pallas as pl
from jax.experimental.pallas import tpu as pltpu
from jax.sharding import PartitionSpec as P

OV = 128

ALPHA = 0.5
BETA = 4.0
FLOOR = 0.5
EPSILON = 1e-06

UP, DOWN, LEFT, RIGHT = 0, 1, 2, 3
CHUNKS = 8
SPLITS = 2


def dft_tables(size_w):
    counter = np.arange(size_w)
    angles = 2.0 * math.pi / size_w * (counter[:, None] * counter[None, :] % size_w)
    both = np.concatenate([np.cos(angles), np.sin(angles)], axis=1) / math.sqrt(size_w)
    both = both.astype(np.float32)
    head = both.astype(jnp.bfloat16)
    rest = (both - head.astype(np.float32)).astype(jnp.bfloat16)
    return head, rest


def halves(value):
    head = value.astype(jnp.bfloat16)
    rest = (value - head.astype(jnp.float32)).astype(jnp.bfloat16)
    return head, rest


def dot(left, right):
    return jnp.dot(left, right, preferred_element_type=jnp.float32)


def left_apply(tab_head, tab_rest, re_part, im_part, sign):
    size = re_part.shape[0]
    head, rest = halves(jnp.concatenate([re_part, im_part], axis=1))
    out = dot(tab_head, head) + dot(tab_head, rest) + dot(tab_rest, head)
    cos_re, cos_im = out[:size, :size], out[:size, size:]
    sin_re, sin_im = out[size:, :size], out[size:, size:]
    return cos_re + sign * sin_im, cos_im - sign * sin_re


def right_apply(re_part, im_part, tab_head, tab_rest, sign):
    size = re_part.shape[0]
    head, rest = halves(jnp.concatenate([re_part, im_part], axis=0))
    out = dot(head, tab_head) + dot(rest, tab_head) + dot(head, tab_rest)
    re_cos, re_sin = out[:size, :size], out[:size, size:]
    im_cos, im_sin = out[size:, :size], out[size:, size:]
    return re_cos + sign * im_sin, im_cos - sign * re_sin


def pick(flag, first, second):
    return jnp.where(flag == 1, first, second)


def keep(flag, value):
    return jnp.where(flag == 1, value, 0.0)


def across(*parts):
    return jnp.concatenate(parts, axis=1)


def stacked(*parts):
    return jnp.concatenate(parts, axis=0)


class Spot:
    def __init__(self, row, col, tile):
        half = tile // 2
        inside = lambda place: jnp.where(
            place < 0, jnp.maximum(place, -OV), jnp.clip(place, half, half + OV)
        )
        row, col = inside(row), inside(col)
        self.row, self.col = row, col
        self.up = jnp.where(row < 0, 1, 0)
        self.left = jnp.where(col < 0, 1, 0)
        self.row_on = jnp.where(row < 0, row + OV, row - half)
        self.col_on = jnp.where(col < 0, col + OV, col - half)


def choose(flag, first, second, tile):
    return Spot(
        jnp.where(flag == 1, first.row, second.row),
        jnp.where(flag == 1, first.col, second.col),
        tile,
    )


def same(first, second):
    return 1 - (first - second) * (first - second)


def kernel(
    rows, cols, pos, order, obj, probe_in, amps_in, lh_in, lr_in, rh_in, rr_in,
    change_out, probe_out,
    own, rim, mid, probe, amps, lh, lr, rh, rr, info, infos, hs, hr, vbuf, placed,
    bs, br, bnd_s, bnd_r, dreg, cs, cr, xs, xr, ws, wr, body_s, body_r, turn_s, turn_r,
    psum, acc, rx0, rx1, red, rx2, res, pw, pw0, pwa, pw1, pw2,
    local_sems, send_sems, recv_sems,
):
    tile = own.shape[2]
    blocks = tile // OV
    size_w = probe.shape[-1]
    half = tile // 2
    span = half + OV
    row, col = lax.axis_index("row"), lax.axis_index("col")
    core, par = row % 2, col % 2
    at = lambda r, c: {"row": r, "col": c}
    above, below = at((row + rows - 1) % rows, col), at((row + 1) % rows, col)
    west, east = at(row, (col + cols - 1) % cols), at(row, (col + 1) % cols)
    partner = at(row, col + 1 - 2 * par)
    onward = at(row, (col + 2 - 4 * par + cols) % cols)
    sibling = at(row + 1 - 2 * core, col)
    used = [0, 0]

    def fetch(source, target):
        copy = pltpu.make_async_copy(source, target, local_sems.at[used[0]])
        used[0] += 1
        copy.start()
        return copy

    def send(source, target, device):
        copy = pltpu.make_async_remote_copy(
            src_ref=source,
            dst_ref=target,
            send_sem=send_sems.at[used[1]],
            recv_sem=recv_sems.at[used[1]],
            device_id=device,
            device_id_type=pl.DeviceIdType.MESH,
        )
        used[1] += 1
        copy.start()
        sent.append(copy)
        return copy

    sent = []
    lanes = [pl.ds(block * OV, OV) for block in range(blocks)]
    own_in = [fetch(obj.at[:, :, lanes[block]], own.at[:, block]) for block in range(blocks)]
    rest_in = [
        fetch(source, target)
        for source, target in (
            (probe_in, probe), (lh_in, lh), (lr_in, lr), (rh_in, rh), (rr_in, rr), (amps_in, amps),
        )
    ]

    mine = []
    for batch in range(2):
        which = order[batch]
        info[2 * batch] = pos[0, which]
        info[2 * batch + 1] = pos[1, which]
        mine.append(Spot(pos[0, which], pos[1, which], tile))

    barrier = pltpu.get_barrier_semaphore()
    peers = [above, below]
    peers += [at(row, (col + d) % cols) for d in range(1, cols)]
    peers += [at((row + 2 * d) % rows, col) for d in range(1, rows // 2)]
    for peer in peers:
        pl.semaphore_signal(barrier, inc=1, device_id=peer, device_id_type=pl.DeviceIdType.MESH)
    pl.semaphore_wait(barrier, len(peers))

    info_in = {}
    for peer, slot in ((west, RIGHT), (east, LEFT), (above, DOWN), (below, UP)):
        info_in[slot] = send(info, infos.at[slot], peer)
    side_block = (0, blocks - 1)
    edge_in, mid_in = [], []

    def send_past(block, tall):
        return [
            send(obj.at[:, pl.ds(0, OV), lanes[block]], tall.at[:, pl.ds(OV + tile, OV), :], above),
            send(obj.at[:, pl.ds(tile - OV, OV), lanes[block]], tall.at[:, pl.ds(0, OV), :], below),
        ]

    for side in range(2):
        edge_in += send_past(side_block[side], rim.at[side])
    for block in range(1, blocks - 1):
        mid_in += send_past(block, mid.at[block - 1])

    for copy in own_in:
        copy.wait()
    for index in range(4):
        for block in range(span // OV):
            gap = jnp.zeros((OV, OV), jnp.float32)
            placed[index, block, pl.ds(0, OV), :] = gap
            placed[index, block, pl.ds(OV + size_w, OV), :] = gap

    near = {}

    def spots(slot):
        info_in[slot].wait_recv()
        near[slot] = [Spot(infos[slot, 2 * b], infos[slot, 2 * b + 1], tile) for b in range(2)]

    spots(LEFT)
    spots(RIGHT)
    west_first = 1 - near[LEFT][0].left
    east_first = near[RIGHT][0].left
    west_spot = choose(west_first, near[LEFT][0], near[LEFT][1], tile)
    east_spot = choose(east_first, near[RIGHT][0], near[RIGHT][1], tile)
    wanted = (west_spot, east_spot)

    halo_in = {}
    for side in range(2):
        spot = wanted[side]
        start = jnp.where(spot.up == 1, spot.row + OV, spot.row)
        for part in range(2):
            hs[side, 0, part] = own[part, side_block[side], pl.ds(start, OV), :]
        halo_in[1 - side, 0] = send(
            hs.at[side, 0], hr.at[1 - side, 0], (west, east)[side]
        )

    for side in range(2):
        for part in range(2):
            rim[side, part, pl.ds(OV, tile), :] = own[part, side_block[side]]
    squares = jnp.zeros((8, OV), jnp.float32)
    for part in range(2):
        for block in range(blocks):
            value = own[part, block]
            if 0 < block < blocks - 1:
                mid[block - 1, part, pl.ds(OV, tile), :] = value
            squares = squares + jnp.sum((value * value).reshape(tile // 8, 8, OV), axis=0)
    pw[...] = squares

    for copy in edge_in:
        copy.wait_recv()
    for side in range(2):
        spot = wanted[side]
        start = jnp.where(spot.up == 1, spot.row + OV, spot.row + 2 * OV)
        for part in range(2):
            hs[side, 1, part] = rim[side, part, pl.ds(start, OV), :]
        halo_in[1 - side, 1] = send(
            hs.at[side, 1], hr.at[1 - side, 1], (west, east)[side]
        )

    for copy in mid_in:
        copy.wait_recv()
    for copy in rest_in:
        copy.wait()
    spots(UP)
    spots(DOWN)
    power_probe = jnp.sum(
        probe[0] * probe[0] + probe[1] * probe[1], axis=(0, 1), keepdims=True
    )
    step_object = ALPHA / (power_probe / float(size_w * size_w) + EPSILON)

    def cut(value, spot):
        back = jnp.where(spot.col_on == 0, 0, span - spot.col_on)
        return pltpu.roll(value, back, 1)[:, :size_w]

    for copy in halo_in.values():
        copy.wait_recv()
    for batch in range(2):
        spot = mine[batch]
        for part in range(2):
            first = pick(spot.left, hr[0, 0, part], hr[1, 0, part])
            second = pick(spot.left, hr[0, 1, part], hr[1, 1, part])
            strip = pick(spot.up, stacked(second, first), stacked(first, second))
            window = pl.ds(spot.row + OV, size_w)
            tall = [rim[0, part, window, :]]
            tall += [mid[block - 1, part, window, :] for block in range(1, blocks - 1)]
            tall.append(rim[1, part, window, :])
            near_half = half // OV
            body = pick(spot.left, across(*tall[:near_half]), across(*tall[near_half:]))
            region = pick(spot.left, across(strip, body), across(body, strip))
            vbuf[2 * batch + part] = cut(region, spot)

    def transform(batch):
        spot = mine[batch]
        win_re, win_im = vbuf[2 * batch], vbuf[2 * batch + 1]
        probe_re, probe_im = probe[0], probe[1]
        exit_re = probe_re * win_re - probe_im * win_im
        exit_im = probe_re * win_im + probe_im * win_re
        half_re, half_im = left_apply(lh[...], lr[...], exit_re, exit_im, 1.0)
        far_re, far_im = right_apply(half_re, half_im, rh[...], rr[...], 1.0)
        modulus = jnp.sqrt(far_re * far_re + far_im * far_im)
        scaled = amps[order[batch]] / jnp.maximum(modulus, FLOOR)
        half_re, half_im = left_apply(
            lh[...], lr[...], far_re - scaled * far_re, far_im - scaled * far_im, -1.0
        )
        back_re, back_im = right_apply(half_re, half_im, rh[...], rr[...], -1.0)
        terms = (
            win_re * back_re + win_im * back_im,
            win_re * back_im - win_im * back_re,
        )
        for part in range(2):
            psum[part] = terms[part] if batch == 0 else psum[part] + terms[part]
        moves = (
            probe_re * back_re + probe_im * back_im,
            probe_re * back_im - probe_im * back_re,
        )
        beside = jnp.zeros((size_w, span - size_w), jnp.float32)
        for part in range(2):
            wide = across(step_object * moves[part], beside)
            wide = pltpu.roll(wide, spot.col_on, 1)
            for block in range(span // OV):
                placed[2 * batch + part, block, pl.ds(OV, size_w), :] = wide[:, block * OV : (block + 1) * OV]

    def load_placed(index, start, count):
        rows_of = pl.ds(start, count)
        return across(*[placed[index, block, rows_of, :] for block in range(span // OV)])

    def frame(batch, part, kind, low=0, count=OV):
        spot = mine[batch]
        upper, lower = {"past": (-OV, tile), "edge": (0, tile - OV), "deep": (OV, half)}[kind]
        start = OV - spot.row + jnp.where(spot.up == 1, upper, lower)
        return load_placed(2 * batch + part, start + low, count)

    transform(0)

    split = 2 * OV // CHUNKS
    per = OV // split
    block_in, block_on = [], []
    spot = mine[0]
    for chunk in range(CHUNKS):
        kind = ("edge", "deep")[chunk // per]
        if chunk % per == 0:
            values = [frame(0, part, kind) for part in range(2)]
            values = [pick(spot.left, v[:, : 2 * OV], v[:, span - 2 * OV :]) for v in values]
        low = (chunk % per) * split
        for part in range(2):
            bs[chunk, part] = values[part][low : low + split]
        block_in.append(send(bs.at[chunk], br.at[par, chunk], partner))
    for part in range(2):
        value = frame(0, part, "past")
        cs[part] = pick(spot.left, value[:, :OV], value[:, span - OV :])
    corner_in = send(cs, cr.at[par], partner)

    def hand_on(copy, buffer, *index):
        copy.wait_recv()
        return send(buffer.at[(1 - par,) + index], buffer.at[(par,) + index], onward)

    def near_block(side, part, kind):
        base = 0 if kind == "edge" else per
        return stacked(*[br[side, base + k, part] for k in range(per)])

    toward = (1 - near[LEFT][0].left, near[RIGHT][0].left)
    blank = jnp.zeros((split, span - 2 * OV), jnp.float32)
    band_in = []

    def send_bands(chunk):
        for way, slot in ((0, UP), (1, DOWN)):
            goal = near[slot][1]
            match = spot.up if way == 0 else 1 - spot.up
            use_own = match * same(spot.left, goal.left)
            ups = [near[LEFT][0].up, near[RIGHT][0].up]
            if way == 1:
                ups = [1 - flag for flag in ups]
            use = jnp.where(goal.left == 1, ups[0] * toward[0], ups[1] * toward[1])
            for part in range(2):
                block = keep(use, pick(goal.left, br[0, chunk, part], br[1, chunk, part]))
                whole = keep(use_own, frame(0, part, "edge", chunk * split, split))
                whole = whole + pick(goal.left, across(block, blank), across(blank, block))
                bnd_s[way, chunk, part] = cut(whole, goal)
            band_in.append(
                send(bnd_s.at[way, chunk], bnd_r.at[1 - way, chunk], (above, below)[way])
            )

    lead = min(3, per)
    for chunk in range(lead):
        block_on.append(hand_on(block_in[chunk], br, chunk))
    for chunk in range(per):
        block_on[chunk].wait_recv()
        send_bands(chunk)
        block_on.append(hand_on(block_in[chunk + lead], br, chunk + lead))
    for chunk in range(per + lead, CHUNKS):
        block_on.append(hand_on(block_in[chunk], br, chunk))
    for copy in block_on[per:]:
        copy.wait_recv()

    spot = mine[1]
    use = jnp.where(
        spot.left == 1,
        toward[0] * same(near[LEFT][0].up, spot.up),
        toward[1] * same(near[RIGHT][0].up, spot.up),
    )
    wide_blank = jnp.zeros((half, span - 2 * OV), jnp.float32)
    inside = []
    for part in range(2):
        at_edge = pick(spot.left, near_block(0, part, "edge"), near_block(1, part, "edge"))
        deep = pick(spot.left, near_block(0, part, "deep"), near_block(1, part, "deep"))
        block = keep(use, pick(spot.up, stacked(at_edge, deep), stacked(deep, at_edge)))
        inside.append(cut(pick(spot.left, across(block, wide_blank), across(wide_blank, block)), spot))
    for copy in band_in:
        copy.wait_recv()
    for part in range(2):
        bands = [pick(spot.up, bnd_r[0, k, part], bnd_r[1, k, part]) for k in range(per)]
        band = stacked(*bands)
        region = pick(spot.up, stacked(band, inside[part]), stacked(inside[part], band))
        for block in range(size_w // OV):
            dreg[part, block] = region[:, block * OV : (block + 1) * OV]
    for part in range(2):
        change = [dreg[part, b, pl.ds(spot.row_on, size_w), :] for b in range(size_w // OV)]
        vbuf[2 + part] = vbuf[2 + part] - across(*change)

    transform(1)

    pair_in = send(psum.at[1 - core], rx0, sibling)
    power_in = [send(pw, pw0, sibling)]

    first_up = mine[0].up
    out_spots = (
        choose(first_up, mine[0], mine[1], tile),
        choose(first_up, mine[1], mine[0], tile),
    )
    out_batch = (1 - first_up, first_up)
    up_start = jnp.maximum(OV - out_spots[0].row, OV)

    def own_half(way, part, start, count):
        value = load_placed(2 * out_batch[way] + part, start, count)
        return pick(out_spots[way].left, value[:, OV:], value[:, :half])

    past_in = []
    for way in range(2):
        start = up_start - OV if way == 0 else OV + tile - out_spots[1].row
        for part in range(2):
            body_s[way, part] = own_half(way, part, start, OV)
        past_in.append(send(body_s.at[way], body_r.at[1 - way], (above, below)[way]))
    spot = mine[1]

    def outer(part, kind, low=0, count=OV):
        value = frame(1, part, kind, low, count)
        return pick(spot.left, value[:, :OV], value[:, span - OV :])

    for part in range(2):
        for chunk in range(per):
            xs[chunk, part] = outer(part, "past", chunk * split, split)
        for index, kind in enumerate(("edge", "deep")):
            ws[index, part] = outer(part, kind)

    pair_in.wait_recv()
    acc[...] = psum[core] + rx0[...]
    power_in[0].wait_recv()
    pwa[...] = pw[...] + pw0[...]
    piece = size_w // cols
    sub = piece // SPLITS

    def slab(place, part):
        return pl.ds(pl.multiple_of(place * piece + part * sub, sub), sub)

    part_in = [[] for _ in range(SPLITS)]
    for half_of in range(SPLITS):
        for step in range(1, cols):
            other = (col + step) % cols
            part_in[half_of].append(
                send(acc.at[slab(other, half_of)], rx1.at[step - 1, half_of], at(row, other))
            )
            if half_of == 0:
                power_in.append(send(pwa, pw1.at[col], at(row, other)))
    corner_on = [hand_on(corner_in, cr)]
    turn_from = [send(xs.at[k], xr.at[par, k], partner) for k in range(per)]
    strip_in = [send(ws.at[k], wr.at[par, k], partner) for k in range(2)]

    plane = row // 2
    plane_in = [[] for _ in range(SPLITS)]
    for half_of in range(SPLITS):
        mine_piece = acc[slab(col, half_of), :]
        for copy in part_in[half_of]:
            copy.wait_recv()
        for step in range(cols - 1):
            mine_piece = mine_piece + rx1[step, half_of]
        red[half_of] = mine_piece
        for step in range(1, rows // 2):
            goal = at((row + 2 * step) % rows, col)
            plane_in[half_of].append(send(red.at[half_of], rx2.at[plane, half_of], goal))
    for copy in power_in[1:]:
        copy.wait_recv()
    pw1[col] = pwa[...]
    total = pw1[0]
    for place in range(1, cols):
        total = total + pw1[place]
    pw2[rows // 2] = total
    for step in range(1, rows // 2):
        goal = at((row + 2 * step) % rows, col)
        plane_in[1].append(send(pw2.at[rows // 2], pw2.at[plane], goal))
    for chunk in range(per):
        corner_on.append(hand_on(turn_from[chunk], xr, chunk))
    for copy in corner_on:
        copy.wait_recv()
    turn_in = []
    for way in range(2):
        for side in range(2):
            theirs, first = wanted[side], (west_first, east_first)[side]
            match = theirs.up if way == 0 else 1 - theirs.up
            for part in range(2):
                fresh = stacked(*[xr[side, k, part] for k in range(per)])
                turn_s[way, side, part] = keep(match, pick(first, cr[side, part], fresh))
        turn_in.append(send(turn_s.at[way], turn_r.at[1 - way], (above, below)[way]))

    strip_on = []
    gather_in, last_in = [[] for _ in range(SPLITS)], []
    for half_of in range(SPLITS):
        for copy in plane_in[half_of]:
            copy.wait_recv()
        rx2[plane, half_of] = red[half_of]
        whole = rx2[0, half_of]
        for place in range(1, rows // 2):
            whole = whole + rx2[place, half_of]
        here = slab(col, half_of)
        res[core, here, :] = whole
        for step in range(1, cols):
            other = at(row, (col + step) % cols)
            gather_in[half_of].append(send(res.at[core, here], res.at[core, here], other))
        last_in.append(send(res.at[core, here], res.at[core, here], sibling))
        strip_on.append(hand_on(strip_in[half_of], wr, half_of))
    pw2[plane] = total
    total = pw2[0]
    for place in range(1, rows // 2):
        total = total + pw2[place]

    for half_of in range(SPLITS):
        for step, copy in enumerate(gather_in[half_of]):
            copy.wait_recv()
            came = slab((col + cols - 1 - step) % cols, half_of)
            last_in.append(send(res.at[core, came], res.at[core, came], sibling))

    for copy in strip_on:
        copy.wait_recv()
    gap = jnp.zeros((half, tile - 2 * OV), jnp.float32)
    changes = []
    for part in range(2):
        strips_of = []
        for side in range(2):
            theirs, first = wanted[side], (west_first, east_first)[side]
            part_of = slice(OV, 2 * OV) if side == 0 else slice(0, OV)
            at_edge = near_block(side, part, "edge")[:, part_of]
            deep = near_block(side, part, "deep")[:, part_of]
            early = pick(theirs.up, stacked(at_edge, deep), stacked(deep, at_edge))
            fresh = pick(
                theirs.up,
                stacked(wr[side, 0, part], wr[side, 1, part]),
                stacked(wr[side, 1, part], wr[side, 0, part]),
            )
            strips_of.append((theirs.up, pick(first, early, fresh)))
        for way in range(2):
            start = up_start if way == 0 else OV + half - out_spots[1].row
            body = own_half(way, part, start, half)
            space = jnp.zeros((half, half), jnp.float32)
            value = pick(out_spots[way].left, across(body, space), across(space, body))
            strips = [keep(up if way == 0 else 1 - up, strip) for up, strip in strips_of]
            changes.append(value + across(strips[0], gap, strips[1]))

    for copy in past_in + turn_in:
        copy.wait_recv()
    gap = jnp.zeros((OV, tile - 2 * OV), jnp.float32)
    space = jnp.zeros((OV, half), jnp.float32)
    rest = jnp.zeros((half - OV, tile), jnp.float32)
    for part in range(2):
        for way in range(2):
            spots_of = near[(UP, DOWN)[way]]
            flag = 1 - spots_of[0].up if way == 0 else spots_of[0].up
            left = jnp.where(flag == 1, spots_of[0].left, spots_of[1].left)
            body = body_r[way, part]
            late = pick(left, across(body, space), across(space, body))
            late = late + across(turn_r[way, 0, part], gap, turn_r[way, 1, part])
            late = stacked(late, rest) if way == 0 else stacked(rest, late)
            change_out[part, pl.ds(way * half, half), :] = changes[2 * part + way] + late

    for copy in last_in:
        copy.wait_recv()
    cell_count = float(tile * tile * rows * cols)
    mean_power = jnp.sum(total, axis=(0, 1), keepdims=True) / cell_count + EPSILON
    step_probe = BETA * size_w * size_w / (cell_count * mean_power)
    for part in range(2):
        probe_out[part] = step_probe * res[part]
    for copy in sent:
        copy.wait_send()


def local(mesh_shape, object_field, probe_field, amplitudes, positions, batch_order):
    rows, cols = mesh_shape["row"], mesh_shape["col"]
    size_w = probe_field.shape[-1]
    tile = object_field.shape[1]
    half = tile // 2
    span = half + OV
    head, rest = dft_tables(size_w)
    f32 = lambda *shape: pltpu.VMEM(shape, jnp.float32)
    b16 = lambda *shape: pltpu.VMEM(shape, jnp.bfloat16)
    piece = size_w // cols
    split = 2 * OV // CHUNKS
    scratch = dict(
        own=f32(2, tile // OV, tile, OV),
        rim=f32(2, 2, tile + 2 * OV, OV),
        mid=f32(tile // OV - 2, 2, tile + 2 * OV, OV),
        probe=f32(2, size_w, size_w),
        amps=f32(2, size_w, size_w),
        lh=b16(2 * size_w, size_w),
        lr=b16(2 * size_w, size_w),
        rh=b16(size_w, 2 * size_w),
        rr=b16(size_w, 2 * size_w),
        info=pltpu.SMEM((4,), jnp.int32),
        infos=pltpu.SMEM((4, 4), jnp.int32),
        hs=f32(2, 2, 2, OV, OV),
        hr=f32(2, 2, 2, OV, OV),
        vbuf=f32(4, size_w, size_w),
        placed=f32(4, span // OV, size_w + 2 * OV, OV),
        bs=f32(CHUNKS, 2, split, 2 * OV),
        br=f32(2, CHUNKS, 2, split, 2 * OV),
        bnd_s=f32(2, OV // split, 2, split, size_w),
        bnd_r=f32(2, OV // split, 2, split, size_w),
        dreg=f32(2, size_w // OV, span, OV),
        cs=f32(2, OV, OV),
        cr=f32(2, 2, OV, OV),
        xs=f32(OV // split, 2, split, OV),
        xr=f32(2, OV // split, 2, split, OV),
        ws=f32(2, 2, OV, OV),
        wr=f32(2, 2, 2, OV, OV),
        body_s=f32(2, 2, OV, half),
        body_r=f32(2, 2, OV, half),
        turn_s=f32(2, 2, 2, OV, OV),
        turn_r=f32(2, 2, 2, OV, OV),
        psum=f32(2, size_w, size_w),
        acc=f32(size_w, size_w),
        rx0=f32(size_w, size_w),
        rx1=f32(cols - 1, SPLITS, piece // SPLITS, size_w),
        red=f32(SPLITS, piece // SPLITS, size_w),
        rx2=f32(rows // 2, SPLITS, piece // SPLITS, size_w),
        res=f32(2, size_w, size_w),
        pw=f32(8, 128),
        pw0=f32(8, 128),
        pwa=f32(8, 128),
        pw1=f32(cols, 8, 128),
        pw2=f32(rows // 2 + 1, 8, 128),
    )
    sends = 96 + 4 * cols + 2 * rows
    hbm = pl.BlockSpec(memory_space=pltpu.HBM)
    vmem = pl.BlockSpec(memory_space=pltpu.VMEM)
    smem = pl.BlockSpec(memory_space=pltpu.SMEM)
    dma = pltpu.SemaphoreType.DMA
    fixed = lambda value: pltpu.with_memory_space_constraint(value, pltpu.HBM)
    change, probe_change = pl.pallas_call(
        functools.partial(kernel, rows, cols),
        out_shape=(
            jax.ShapeDtypeStruct(object_field.shape, jnp.float32),
            jax.ShapeDtypeStruct(probe_field.shape, jnp.float32),
        ),
        in_specs=[smem, smem] + [hbm] * 7,
        out_specs=(vmem, vmem),
        scratch_shapes=list(scratch.values()) + [dma((32,)), dma((sends,)), dma((sends,))],
        compiler_params=pltpu.CompilerParams(
            collective_id=0, has_side_effects=True, vmem_limit_bytes=36 * 1024 * 1024
        ),
    )(
        fixed(positions[0, 0]),
        fixed(batch_order[0, 0]),
        fixed(object_field),
        fixed(probe_field),
        fixed(amplitudes[0, 0]),
        fixed(jnp.asarray(np.concatenate(np.split(head, 2, axis=1), axis=0))),
        fixed(jnp.asarray(np.concatenate(np.split(rest, 2, axis=1), axis=0))),
        fixed(jnp.asarray(head)),
        fixed(jnp.asarray(rest)),
    )
    return object_field - change, probe_field - probe_change


def solution(mesh):
    return jax.shard_map(
        functools.partial(local, dict(mesh.shape)),
        mesh=mesh,
        in_specs=(
            P(None, "row", "col"),
            P(),
            P("row", "col", None, None, None),
            P("row", "col", None, None),
            P("row", "col", None),
        ),
        out_specs=(P(None, "row", "col"), P()),
        check_vma=False,
    )
```

```python
import functools
import math

import jax
import jax.numpy as jnp
import numpy as np
from jax import lax
from jax.experimental import pallas as pl
from jax.experimental.pallas import tpu as pltpu
from jax.sharding import PartitionSpec as P

OV = 128

ALPHA = 0.5
BETA = 4.0
FLOOR = 0.5
EPSILON = 1e-06

UP, DOWN, LEFT, RIGHT = 0, 1, 2, 3
CHUNKS = 8
SPLITS = 2


def dft_tables(size_w):
    counter = np.arange(size_w)
    angles = 2.0 * math.pi / size_w * (counter[:, None] * counter[None, :] % size_w)
    both = np.concatenate([np.cos(angles), np.sin(angles)], axis=1) / math.sqrt(size_w)
    both = both.astype(np.float32)
    head = both.astype(jnp.bfloat16)
    rest = (both - head.astype(np.float32)).astype(jnp.bfloat16)
    return head, rest


def halves(value):
    head = value.astype(jnp.bfloat16)
    rest = (value - head.astype(jnp.float32)).astype(jnp.bfloat16)
    return head, rest


def dot(left, right):
    return jnp.dot(left, right, preferred_element_type=jnp.float32)


def left_apply(tab_head, tab_rest, re_part, im_part, sign):
    size = re_part.shape[0]
    head, rest = halves(jnp.concatenate([re_part, im_part], axis=1))
    out = dot(tab_head, head) + dot(tab_head, rest) + dot(tab_rest, head)
    cos_re, cos_im = out[:size, :size], out[:size, size:]
    sin_re, sin_im = out[size:, :size], out[size:, size:]
    return cos_re + sign * sin_im, cos_im - sign * sin_re


def right_apply(re_part, im_part, tab_head, tab_rest, sign):
    size = re_part.shape[0]
    head, rest = halves(jnp.concatenate([re_part, im_part], axis=0))
    out = dot(head, tab_head) + dot(rest, tab_head) + dot(head, tab_rest)
    re_cos, re_sin = out[:size, :size], out[:size, size:]
    im_cos, im_sin = out[size:, :size], out[size:, size:]
    return re_cos + sign * im_sin, im_cos - sign * re_sin


def pick(flag, first, second):
    return jnp.where(flag == 1, first, second)


def keep(flag, value):
    return jnp.where(flag == 1, value, 0.0)


def across(*parts):
    return jnp.concatenate(parts, axis=1)


def stacked(*parts):
    return jnp.concatenate(parts, axis=0)


class Spot:
    def __init__(self, row, col, tile):
        half = tile // 2
        inside = lambda place: jnp.where(
            place < 0, jnp.maximum(place, -OV), jnp.clip(place, half, half + OV)
        )
        row, col = inside(row), inside(col)
        self.row, self.col = row, col
        self.up = jnp.where(row < 0, 1, 0)
        self.left = jnp.where(col < 0, 1, 0)
        self.row_on = jnp.where(row < 0, row + OV, row - half)
        self.col_on = jnp.where(col < 0, col + OV, col - half)


def choose(flag, first, second, tile):
    return Spot(
        jnp.where(flag == 1, first.row, second.row),
        jnp.where(flag == 1, first.col, second.col),
        tile,
    )


def same(first, second):
    return 1 - (first - second) * (first - second)


def kernel(
    rows, cols, pos, order, obj, probe_in, amps_in, lh_in, lr_in, rh_in, rr_in,
    change_out, probe_out,
    own, rim, mid, probe, amps, lh, lr, rh, rr, info, infos, hs, hr, vbuf, placed,
    bs, br, bnd_s, bnd_r, dreg, cs, cr, xs, xr, ws, wr, body_s, body_r, turn_s, turn_r,
    psum, acc, rx0, rx1, red, rx2, res, pw, pw0, pwa, pw1, pw2,
    local_sems, send_sems, recv_sems,
):
    tile = own.shape[2]
    blocks = tile // OV
    size_w = probe.shape[-1]
    half = tile // 2
    span = half + OV
    row, col = lax.axis_index("row"), lax.axis_index("col")
    core, par = row % 2, col % 2
    at = lambda r, c: {"row": r, "col": c}
    above, below = at((row + rows - 1) % rows, col), at((row + 1) % rows, col)
    west, east = at(row, (col + cols - 1) % cols), at(row, (col + 1) % cols)
    partner = at(row, col + 1 - 2 * par)
    onward = at(row, (col + 2 - 4 * par + cols) % cols)
    sibling = at(row + 1 - 2 * core, col)
    used = [0, 0]

    def fetch(source, target):
        copy = pltpu.make_async_copy(source, target, local_sems.at[used[0]])
        used[0] += 1
        copy.start()
        return copy

    def send(source, target, device):
        copy = pltpu.make_async_remote_copy(
            src_ref=source,
            dst_ref=target,
            send_sem=send_sems.at[used[1]],
            recv_sem=recv_sems.at[used[1]],
            device_id=device,
            device_id_type=pl.DeviceIdType.MESH,
        )
        used[1] += 1
        copy.start()
        sent.append(copy)
        return copy

    sent = []
    lanes = [pl.ds(block * OV, OV) for block in range(blocks)]
    own_in = [fetch(obj.at[:, :, lanes[block]], own.at[:, block]) for block in range(blocks)]
    rest_in = [
        fetch(source, target)
        for source, target in (
            (probe_in, probe), (lh_in, lh), (lr_in, lr), (rh_in, rh), (rr_in, rr), (amps_in, amps),
        )
    ]

    mine = []
    for batch in range(2):
        which = order[batch]
        info[2 * batch] = pos[0, which]
        info[2 * batch + 1] = pos[1, which]
        mine.append(Spot(pos[0, which], pos[1, which], tile))

    barrier = pltpu.get_barrier_semaphore()
    peers = [above, below]
    peers += [at(row, (col + d) % cols) for d in range(1, cols)]
    peers += [at((row + 2 * d) % rows, col) for d in range(1, rows // 2)]
    for peer in peers:
        pl.semaphore_signal(barrier, inc=1, device_id=peer, device_id_type=pl.DeviceIdType.MESH)
    pl.semaphore_wait(barrier, len(peers))

    info_in = {}
    for peer, slot in ((west, RIGHT), (east, LEFT), (above, DOWN), (below, UP)):
        info_in[slot] = send(info, infos.at[slot], peer)
    side_block = (0, blocks - 1)
    edge_in, mid_in = [], []

    def send_past(block, tall):
        return [
            send(obj.at[:, pl.ds(0, OV), lanes[block]], tall.at[:, pl.ds(OV + tile, OV), :], above),
            send(obj.at[:, pl.ds(tile - OV, OV), lanes[block]], tall.at[:, pl.ds(0, OV), :], below),
        ]

    for side in range(2):
        edge_in += send_past(side_block[side], rim.at[side])
    for block in range(1, blocks - 1):
        mid_in += send_past(block, mid.at[block - 1])

    for copy in own_in:
        copy.wait()
    for index in range(4):
        for block in range(span // OV):
            gap = jnp.zeros((OV, OV), jnp.float32)
            placed[index, block, pl.ds(0, OV), :] = gap
            placed[index, block, pl.ds(OV + size_w, OV), :] = gap

    near = {}

    def spots(slot):
        info_in[slot].wait_recv()
        near[slot] = [Spot(infos[slot, 2 * b], infos[slot, 2 * b + 1], tile) for b in range(2)]

    spots(LEFT)
    spots(RIGHT)
    west_first = 1 - near[LEFT][0].left
    east_first = near[RIGHT][0].left
    west_spot = choose(west_first, near[LEFT][0], near[LEFT][1], tile)
    east_spot = choose(east_first, near[RIGHT][0], near[RIGHT][1], tile)
    wanted = (west_spot, east_spot)

    halo_in = {}
    for side in range(2):
        spot = wanted[side]
        start = jnp.where(spot.up == 1, spot.row + OV, spot.row)
        for part in range(2):
            hs[side, 0, part] = own[part, side_block[side], pl.ds(start, OV), :]
        halo_in[1 - side, 0] = send(
            hs.at[side, 0], hr.at[1 - side, 0], (west, east)[side]
        )

    for side in range(2):
        for part in range(2):
            rim[side, part, pl.ds(OV, tile), :] = own[part, side_block[side]]
    squares = jnp.zeros((8, OV), jnp.float32)
    for part in range(2):
        for block in range(blocks):
            value = own[part, block]
            if 0 < block < blocks - 1:
                mid[block - 1, part, pl.ds(OV, tile), :] = value
            squares = squares + jnp.sum((value * value).reshape(tile // 8, 8, OV), axis=0)
    pw[...] = squares

    for copy in edge_in:
        copy.wait_recv()
    for side in range(2):
        spot = wanted[side]
        start = jnp.where(spot.up == 1, spot.row + OV, spot.row + 2 * OV)
        for part in range(2):
            hs[side, 1, part] = rim[side, part, pl.ds(start, OV), :]
        halo_in[1 - side, 1] = send(
            hs.at[side, 1], hr.at[1 - side, 1], (west, east)[side]
        )

    for copy in mid_in:
        copy.wait_recv()
    for copy in rest_in:
        copy.wait()
    spots(UP)
    spots(DOWN)
    power_probe = jnp.sum(
        probe[0] * probe[0] + probe[1] * probe[1], axis=(0, 1), keepdims=True
    )
    step_object = ALPHA / (power_probe / float(size_w * size_w) + EPSILON)

    def cut(value, spot):
        back = jnp.where(spot.col_on == 0, 0, span - spot.col_on)
        return pltpu.roll(value, back, 1)[:, :size_w]

    for copy in halo_in.values():
        copy.wait_recv()
    for batch in range(2):
        spot = mine[batch]
        for part in range(2):
            first = pick(spot.left, hr[0, 0, part], hr[1, 0, part])
            second = pick(spot.left, hr[0, 1, part], hr[1, 1, part])
            strip = pick(spot.up, stacked(second, first), stacked(first, second))
            window = pl.ds(spot.row + OV, size_w)
            tall = [rim[0, part, window, :]]
            tall += [mid[block - 1, part, window, :] for block in range(1, blocks - 1)]
            tall.append(rim[1, part, window, :])
            near_half = half // OV
            body = pick(spot.left, across(*tall[:near_half]), across(*tall[near_half:]))
            region = pick(spot.left, across(strip, body), across(body, strip))
            vbuf[2 * batch + part] = cut(region, spot)

    def transform(batch):
        spot = mine[batch]
        win_re, win_im = vbuf[2 * batch], vbuf[2 * batch + 1]
        probe_re, probe_im = probe[0], probe[1]
        exit_re = probe_re * win_re - probe_im * win_im
        exit_im = probe_re * win_im + probe_im * win_re
        half_re, half_im = left_apply(lh[...], lr[...], exit_re, exit_im, 1.0)
        far_re, far_im = right_apply(half_re, half_im, rh[...], rr[...], 1.0)
        modulus = jnp.sqrt(far_re * far_re + far_im * far_im)
        scaled = amps[order[batch]] / jnp.maximum(modulus, FLOOR)
        half_re, half_im = left_apply(
            lh[...], lr[...], far_re - scaled * far_re, far_im - scaled * far_im, -1.0
        )
        back_re, back_im = right_apply(half_re, half_im, rh[...], rr[...], -1.0)
        terms = (
            win_re * back_re + win_im * back_im,
            win_re * back_im - win_im * back_re,
        )
        for part in range(2):
            psum[part] = terms[part] if batch == 0 else psum[part] + terms[part]
        moves = (
            probe_re * back_re + probe_im * back_im,
            probe_re * back_im - probe_im * back_re,
        )
        beside = jnp.zeros((size_w, span - size_w), jnp.float32)
        for part in range(2):
            wide = across(step_object * moves[part], beside)
            wide = pltpu.roll(wide, spot.col_on, 1)
            for block in range(span // OV):
                placed[2 * batch + part, block, pl.ds(OV, size_w), :] = wide[:, block * OV : (block + 1) * OV]

    def load_placed(index, start, count):
        rows_of = pl.ds(start, count)
        return across(*[placed[index, block, rows_of, :] for block in range(span // OV)])

    def frame(batch, part, kind, low=0, count=OV):
        spot = mine[batch]
        upper, lower = {"past": (-OV, tile), "edge": (0, tile - OV), "deep": (OV, half)}[kind]
        start = OV - spot.row + jnp.where(spot.up == 1, upper, lower)
        return load_placed(2 * batch + part, start + low, count)

    transform(0)

    split = 2 * OV // CHUNKS
    per = OV // split
    block_in, block_on = [], []
    spot = mine[0]
    for chunk in range(CHUNKS):
        kind = ("edge", "deep")[chunk // per]
        if chunk % per == 0:
            values = [frame(0, part, kind) for part in range(2)]
            values = [pick(spot.left, v[:, : 2 * OV], v[:, span - 2 * OV :]) for v in values]
        low = (chunk % per) * split
        for part in range(2):
            bs[chunk, part] = values[part][low : low + split]
        block_in.append(send(bs.at[chunk], br.at[par, chunk], partner))
    for part in range(2):
        value = frame(0, part, "past")
        cs[part] = pick(spot.left, value[:, :OV], value[:, span - OV :])
    corner_in = send(cs, cr.at[par], partner)

    def hand_on(copy, buffer, *index):
        copy.wait_recv()
        return send(buffer.at[(1 - par,) + index], buffer.at[(par,) + index], onward)

    def near_block(side, part, kind):
        base = 0 if kind == "edge" else per
        return stacked(*[br[side, base + k, part] for k in range(per)])

    toward = (1 - near[LEFT][0].left, near[RIGHT][0].left)
    blank = jnp.zeros((split, span - 2 * OV), jnp.float32)
    band_in = []

    def send_bands(chunk):
        for way, slot in ((0, UP), (1, DOWN)):
            goal = near[slot][1]
            match = spot.up if way == 0 else 1 - spot.up
            use_own = match * same(spot.left, goal.left)
            ups = [near[LEFT][0].up, near[RIGHT][0].up]
            if way == 1:
                ups = [1 - flag for flag in ups]
            use = jnp.where(goal.left == 1, ups[0] * toward[0], ups[1] * toward[1])
            for part in range(2):
                block = keep(use, pick(goal.left, br[0, chunk, part], br[1, chunk, part]))
                whole = keep(use_own, frame(0, part, "edge", chunk * split, split))
                whole = whole + pick(goal.left, across(block, blank), across(blank, block))
                bnd_s[way, chunk, part] = cut(whole, goal)
            band_in.append(
                send(bnd_s.at[way, chunk], bnd_r.at[1 - way, chunk], (above, below)[way])
            )

    lead = min(3, per)
    for chunk in range(lead):
        block_on.append(hand_on(block_in[chunk], br, chunk))
    for chunk in range(per):
        block_on[chunk].wait_recv()
        send_bands(chunk)
        block_on.append(hand_on(block_in[chunk + lead], br, chunk + lead))
    for chunk in range(per + lead, CHUNKS):
        block_on.append(hand_on(block_in[chunk], br, chunk))
    for copy in block_on[per:]:
        copy.wait_recv()

    spot = mine[1]
    use = jnp.where(
        spot.left == 1,
        toward[0] * same(near[LEFT][0].up, spot.up),
        toward[1] * same(near[RIGHT][0].up, spot.up),
    )
    wide_blank = jnp.zeros((half, span - 2 * OV), jnp.float32)
    inside = []
    for part in range(2):
        at_edge = pick(spot.left, near_block(0, part, "edge"), near_block(1, part, "edge"))
        deep = pick(spot.left, near_block(0, part, "deep"), near_block(1, part, "deep"))
        block = keep(use, pick(spot.up, stacked(at_edge, deep), stacked(deep, at_edge)))
        inside.append(cut(pick(spot.left, across(block, wide_blank), across(wide_blank, block)), spot))
    for copy in band_in:
        copy.wait_recv()
    for part in range(2):
        bands = [pick(spot.up, bnd_r[0, k, part], bnd_r[1, k, part]) for k in range(per)]
        band = stacked(*bands)
        region = pick(spot.up, stacked(band, inside[part]), stacked(inside[part], band))
        for block in range(size_w // OV):
            dreg[part, block] = region[:, block * OV : (block + 1) * OV]
    for part in range(2):
        change = [dreg[part, b, pl.ds(spot.row_on, size_w), :] for b in range(size_w // OV)]
        vbuf[2 + part] = vbuf[2 + part] - across(*change)

    transform(1)

    pair_in = send(psum.at[1 - core], rx0, sibling)
    power_in = [send(pw, pw0, sibling)]

    pair_in.wait_recv()
    acc[...] = psum[core] + rx0[...]
    power_in[0].wait_recv()
    pwa[...] = pw[...] + pw0[...]
    piece = size_w // cols
    sub = piece // SPLITS

    def slab(place, part):
        return pl.ds(pl.multiple_of(place * piece + part * sub, sub), sub)

    part_in = [[] for _ in range(SPLITS)]
    for half_of in range(SPLITS):
        for step in range(1, cols):
            other = (col + step) % cols
            part_in[half_of].append(
                send(acc.at[slab(other, half_of)], rx1.at[step - 1, half_of], at(row, other))
            )
            if half_of == 0:
                power_in.append(send(pwa, pw1.at[col], at(row, other)))
    corner_on = [hand_on(corner_in, cr)]

    first_up = mine[0].up
    out_spots = (
        choose(first_up, mine[0], mine[1], tile),
        choose(first_up, mine[1], mine[0], tile),
    )
    out_batch = (1 - first_up, first_up)
    up_start = jnp.maximum(OV - out_spots[0].row, OV)

    def own_half(way, part, start, count):
        value = load_placed(2 * out_batch[way] + part, start, count)
        return pick(out_spots[way].left, value[:, OV:], value[:, :half])

    spot = mine[1]

    def outer(part, kind, low=0, count=OV):
        value = frame(1, part, kind, low, count)
        return pick(spot.left, value[:, :OV], value[:, span - OV :])

    for part in range(2):
        for chunk in range(per):
            xs[chunk, part] = outer(part, "past", chunk * split, split)
    turn_from = [send(xs.at[k], xr.at[par, k], partner) for k in range(per)]
    for part in range(2):
        for index, kind in enumerate(("edge", "deep")):
            ws[index, part] = outer(part, kind)
    strip_in = [send(ws.at[k], wr.at[par, k], partner) for k in range(2)]
    past_in = []
    for way in range(2):
        start = up_start - OV if way == 0 else OV + tile - out_spots[1].row
        for part in range(2):
            body_s[way, part] = own_half(way, part, start, OV)
        past_in.append(send(body_s.at[way], body_r.at[1 - way], (above, below)[way]))

    plane = row // 2
    plane_in = [[] for _ in range(SPLITS)]
    for half_of in range(SPLITS):
        mine_piece = acc[slab(col, half_of), :]
        for copy in part_in[half_of]:
            copy.wait_recv()
        for step in range(cols - 1):
            mine_piece = mine_piece + rx1[step, half_of]
        red[half_of] = mine_piece
        for step in range(1, rows // 2):
            goal = at((row + 2 * step) % rows, col)
            plane_in[half_of].append(send(red.at[half_of], rx2.at[plane, half_of], goal))
    for copy in power_in[1:]:
        copy.wait_recv()
    pw1[col] = pwa[...]
    total = pw1[0]
    for place in range(1, cols):
        total = total + pw1[place]
    pw2[rows // 2] = total
    for step in range(1, rows // 2):
        goal = at((row + 2 * step) % rows, col)
        plane_in[1].append(send(pw2.at[rows // 2], pw2.at[plane], goal))
    for chunk in range(per):
        corner_on.append(hand_on(turn_from[chunk], xr, chunk))
    turn_in = []

    def send_turns():
        for copy in corner_on:
            copy.wait_recv()
        for way in range(2):
            for side in range(2):
                theirs, first = wanted[side], (west_first, east_first)[side]
                match = theirs.up if way == 0 else 1 - theirs.up
                for part in range(2):
                    fresh = stacked(*[xr[side, k, part] for k in range(per)])
                    turn_s[way, side, part] = keep(match, pick(first, cr[side, part], fresh))
            turn_in.append(send(turn_s.at[way], turn_r.at[1 - way], (above, below)[way]))

    strip_on = []
    gather_in, last_in = [[] for _ in range(SPLITS)], []
    for half_of in range(SPLITS):
        for copy in plane_in[half_of]:
            copy.wait_recv()
        rx2[plane, half_of] = red[half_of]
        whole = rx2[0, half_of]
        for place in range(1, rows // 2):
            whole = whole + rx2[place, half_of]
        here = slab(col, half_of)
        res[core, here, :] = whole
        for step in range(1, cols):
            other = at(row, (col + step) % cols)
            gather_in[half_of].append(send(res.at[core, here], res.at[core, here], other))
        last_in.append(send(res.at[core, here], res.at[core, here], sibling))
        if half_of == 0:
            send_turns()
    for half_of in range(2):
        strip_on.append(hand_on(strip_in[half_of], wr, half_of))
    pw2[plane] = total
    total = pw2[0]
    for place in range(1, rows // 2):
        total = total + pw2[place]

    for half_of in range(SPLITS):
        for step, copy in enumerate(gather_in[half_of]):
            copy.wait_recv()
            came = slab((col + cols - 1 - step) % cols, half_of)
            last_in.append(send(res.at[core, came], res.at[core, came], sibling))

    for copy in strip_on:
        copy.wait_recv()
    gap = jnp.zeros((half, tile - 2 * OV), jnp.float32)
    changes = []
    for part in range(2):
        strips_of = []
        for side in range(2):
            theirs, first = wanted[side], (west_first, east_first)[side]
            part_of = slice(OV, 2 * OV) if side == 0 else slice(0, OV)
            at_edge = near_block(side, part, "edge")[:, part_of]
            deep = near_block(side, part, "deep")[:, part_of]
            early = pick(theirs.up, stacked(at_edge, deep), stacked(deep, at_edge))
            fresh = pick(
                theirs.up,
                stacked(wr[side, 0, part], wr[side, 1, part]),
                stacked(wr[side, 1, part], wr[side, 0, part]),
            )
            strips_of.append((theirs.up, pick(first, early, fresh)))
        for way in range(2):
            start = up_start if way == 0 else OV + half - out_spots[1].row
            body = own_half(way, part, start, half)
            space = jnp.zeros((half, half), jnp.float32)
            value = pick(out_spots[way].left, across(body, space), across(space, body))
            strips = [keep(up if way == 0 else 1 - up, strip) for up, strip in strips_of]
            changes.append(value + across(strips[0], gap, strips[1]))

    for copy in past_in + turn_in:
        copy.wait_recv()
    gap = jnp.zeros((OV, tile - 2 * OV), jnp.float32)
    space = jnp.zeros((OV, half), jnp.float32)
    rest = jnp.zeros((half - OV, tile), jnp.float32)
    for part in range(2):
        for way in range(2):
            spots_of = near[(UP, DOWN)[way]]
            flag = 1 - spots_of[0].up if way == 0 else spots_of[0].up
            left = jnp.where(flag == 1, spots_of[0].left, spots_of[1].left)
            body = body_r[way, part]
            late = pick(left, across(body, space), across(space, body))
            late = late + across(turn_r[way, 0, part], gap, turn_r[way, 1, part])
            late = stacked(late, rest) if way == 0 else stacked(rest, late)
            change_out[part, pl.ds(way * half, half), :] = changes[2 * part + way] + late

    for copy in last_in:
        copy.wait_recv()
    cell_count = float(tile * tile * rows * cols)
    mean_power = jnp.sum(total, axis=(0, 1), keepdims=True) / cell_count + EPSILON
    step_probe = BETA * size_w * size_w / (cell_count * mean_power)
    for part in range(2):
        probe_out[part] = step_probe * res[part]
    for copy in sent:
        copy.wait_send()


def local(mesh_shape, object_field, probe_field, amplitudes, positions, batch_order):
    rows, cols = mesh_shape["row"], mesh_shape["col"]
    size_w = probe_field.shape[-1]
    tile = object_field.shape[1]
    half = tile // 2
    span = half + OV
    head, rest = dft_tables(size_w)
    f32 = lambda *shape: pltpu.VMEM(shape, jnp.float32)
    b16 = lambda *shape: pltpu.VMEM(shape, jnp.bfloat16)
    piece = size_w // cols
    split = 2 * OV // CHUNKS
    scratch = dict(
        own=f32(2, tile // OV, tile, OV),
        rim=f32(2, 2, tile + 2 * OV, OV),
        mid=f32(tile // OV - 2, 2, tile + 2 * OV, OV),
        probe=f32(2, size_w, size_w),
        amps=f32(2, size_w, size_w),
        lh=b16(2 * size_w, size_w),
        lr=b16(2 * size_w, size_w),
        rh=b16(size_w, 2 * size_w),
        rr=b16(size_w, 2 * size_w),
        info=pltpu.SMEM((4,), jnp.int32),
        infos=pltpu.SMEM((4, 4), jnp.int32),
        hs=f32(2, 2, 2, OV, OV),
        hr=f32(2, 2, 2, OV, OV),
        vbuf=f32(4, size_w, size_w),
        placed=f32(4, span // OV, size_w + 2 * OV, OV),
        bs=f32(CHUNKS, 2, split, 2 * OV),
        br=f32(2, CHUNKS, 2, split, 2 * OV),
        bnd_s=f32(2, OV // split, 2, split, size_w),
        bnd_r=f32(2, OV // split, 2, split, size_w),
        dreg=f32(2, size_w // OV, span, OV),
        cs=f32(2, OV, OV),
        cr=f32(2, 2, OV, OV),
        xs=f32(OV // split, 2, split, OV),
        xr=f32(2, OV // split, 2, split, OV),
        ws=f32(2, 2, OV, OV),
        wr=f32(2, 2, 2, OV, OV),
        body_s=f32(2, 2, OV, half),
        body_r=f32(2, 2, OV, half),
        turn_s=f32(2, 2, 2, OV, OV),
        turn_r=f32(2, 2, 2, OV, OV),
        psum=f32(2, size_w, size_w),
        acc=f32(size_w, size_w),
        rx0=f32(size_w, size_w),
        rx1=f32(cols - 1, SPLITS, piece // SPLITS, size_w),
        red=f32(SPLITS, piece // SPLITS, size_w),
        rx2=f32(rows // 2, SPLITS, piece // SPLITS, size_w),
        res=f32(2, size_w, size_w),
        pw=f32(8, 128),
        pw0=f32(8, 128),
        pwa=f32(8, 128),
        pw1=f32(cols, 8, 128),
        pw2=f32(rows // 2 + 1, 8, 128),
    )
    sends = 96 + 4 * cols + 2 * rows
    hbm = pl.BlockSpec(memory_space=pltpu.HBM)
    vmem = pl.BlockSpec(memory_space=pltpu.VMEM)
    smem = pl.BlockSpec(memory_space=pltpu.SMEM)
    dma = pltpu.SemaphoreType.DMA
    fixed = lambda value: pltpu.with_memory_space_constraint(value, pltpu.HBM)
    change, probe_change = pl.pallas_call(
        functools.partial(kernel, rows, cols),
        out_shape=(
            jax.ShapeDtypeStruct(object_field.shape, jnp.float32),
            jax.ShapeDtypeStruct(probe_field.shape, jnp.float32),
        ),
        in_specs=[smem, smem] + [hbm] * 7,
        out_specs=(vmem, vmem),
        scratch_shapes=list(scratch.values()) + [dma((32,)), dma((sends,)), dma((sends,))],
        compiler_params=pltpu.CompilerParams(
            collective_id=0, has_side_effects=True, vmem_limit_bytes=36 * 1024 * 1024
        ),
    )(
        fixed(positions[0, 0]),
        fixed(batch_order[0, 0]),
        fixed(object_field),
        fixed(probe_field),
        fixed(amplitudes[0, 0]),
        fixed(jnp.asarray(np.concatenate(np.split(head, 2, axis=1), axis=0))),
        fixed(jnp.asarray(np.concatenate(np.split(rest, 2, axis=1), axis=0))),
        fixed(jnp.asarray(head)),
        fixed(jnp.asarray(rest)),
    )
    return object_field - change, probe_field - probe_change


def solution(mesh):
    return jax.shard_map(
        functools.partial(local, dict(mesh.shape)),
        mesh=mesh,
        in_specs=(
            P(None, "row", "col"),
            P(),
            P("row", "col", None, None, None),
            P("row", "col", None, None),
            P("row", "col", None),
        ),
        out_specs=(P(None, "row", "col"), P()),
        check_vma=False,
    )
```
